32 devices in a mesh: ta: 2 (over x), gx: 16 (over z, y, core).
Axes of the slice: x: 2, y: 2, z: 4, core: 2. Of those that a mesh axis runs over, the one named last changes fastest.
Arguments:
- voltages: bfloat16 [2, 128, 2, 256, 512], P('ta', 'gx'), may hold values from -6 to 6
- weights: bfloat16 [2, 256, 2, 512, 64], P(None, 'gx'), may hold values from -0.125 to 0.125
Outputs:
- spectra: float32 [256, 2, 512, 64], P(None, None, 'gx', 'ta')
The draws below stay inside these ranges and needn't reach their ends.
All inputs are finite; a program needn't handle non-finite values.
Results may differ from the reference program's by a relative error of at most 0.0003.
Values may be sent and summed in bfloat16 or wider, within the bound.
A program may use at most 64 MiB of HBM per device.

```python
import jax
import jax.numpy as jnp
from jax import lax

ANTENNA_COUNT = 64
BEAM_TOTAL = 512
CHANNEL_COUNT = 512
HALF_SAMPLES = 512


def block_levels(own_key, shape, cuts, low, largest):
    factor_of = 1.0
    for position, blocks in cuts:
        draws = jax.random.uniform(jax.random.fold_in(jax.random.fold_in(own_key, 6), position), (blocks,), jnp.float32, low / len(cuts), largest / len(cuts))
        factor_of = factor_of * jnp.repeat(jnp.exp(draws), shape[position] // blocks).reshape((-1,) + (1,) * (len(shape) - 1 - position))
    return factor_of


def normal_values(rng, dims, scale, most, pieces=(), dtype=jnp.bfloat16):
    array = scale * jax.random.normal(rng, dims, jnp.float32)
    if pieces:
        array = array * block_levels(rng, dims, pieces, -0.22, 0.18)
    return jnp.clip(array, -most, most).astype(dtype)


def setup_inputs(seed: int = 0) -> dict:
    streams_of = jax.random.split(jax.random.key(seed), 3)
    voltages = normal_values(streams_of[0], (2, 2 * ANTENNA_COUNT, 2, CHANNEL_COUNT // 2, HALF_SAMPLES), 1.0, 6.0, ((0, 2), (1, 16)))
    weights = normal_values(streams_of[1], (2, CHANNEL_COUNT // 2, 2, BEAM_TOTAL, ANTENNA_COUNT), (32 * ANTENNA_COUNT) ** -0.5, 0.125, ((1, 16),))
    return dict(voltages=voltages, weights=weights)


def beam_power(voltage, weight_block):
    antennas = weight_block.shape[3]
    beam_count = weight_block.shape[2]
    powers = []
    for side_index in range(2):
        real_w = weight_block[side_index, 0]
        imag_w = weight_block[side_index, 1]
        upper_rows = jnp.stack([real_w, -imag_w], axis=-1).reshape(beam_count, 2 * antennas)
        bottom_half_rows = jnp.stack([imag_w, real_w], axis=-1).reshape(beam_count, 2 * antennas)
        matrix = jnp.concatenate([upper_rows, bottom_half_rows], 0)
        signal = voltage[side_index * antennas:(side_index + 1) * antennas].reshape(2 * antennas, -1)
        beam_voltage_field = jnp.dot(matrix, signal, preferred_element_type=jnp.float32)
        power = beam_voltage_field[:beam_count] * beam_voltage_field[:beam_count] + beam_voltage_field[beam_count:] * beam_voltage_field[beam_count:]
        powers.append(power.reshape(beam_count, -1, 8).sum(-1))
    return jnp.stack(powers, 0)


def reference(voltages, weights):
    moved = jnp.moveaxis(voltages, 3, 0)
    weight_moved = jnp.moveaxis(weights, 1, 0)

    def one_channel(paired):
        voltage, weight_block = paired
        return beam_power(voltage[0], weight_block) + beam_power(voltage[1], weight_block)

    return lax.map(one_channel, (moved, weight_moved))
```

```python
import functools

import jax
import jax.numpy as jnp
from jax import lax
from jax.experimental import pallas as pl
from jax.experimental.pallas import tpu as pltpu
from jax.sharding import PartitionSpec as P

MESH = pl.DeviceIdType.MESH
CHUNKS = 4


def beam_power(voltage, weight_block):
    antennas = weight_block.shape[3]
    beam_count = weight_block.shape[2]
    powers = []
    for side_index in range(2):
        real_w = weight_block[side_index, 0]
        imag_w = weight_block[side_index, 1]
        upper_rows = jnp.stack([real_w, -imag_w], axis=-1).reshape(beam_count, 2 * antennas)
        bottom_half_rows = jnp.stack([imag_w, real_w], axis=-1).reshape(beam_count, 2 * antennas)
        matrix = jnp.concatenate([upper_rows, bottom_half_rows], 0)
        signal = voltage[side_index * antennas : (side_index + 1) * antennas].reshape(
            2 * antennas, -1
        )
        beam_voltage_field = jnp.dot(matrix, signal, preferred_element_type=jnp.float32)
        power = (
            beam_voltage_field[:beam_count] * beam_voltage_field[:beam_count]
            + beam_voltage_field[beam_count:] * beam_voltage_field[beam_count:]
        )
        powers.append(power.reshape(beam_count, -1, 8).sum(-1))
    return jnp.stack(powers, 0)


def channel_powers(turned, weights):

    def one_channel(column):
        voltage = lax.dynamic_index_in_dim(turned, column, 2, keepdims=False)
        weight_block = lax.dynamic_index_in_dim(weights, column, 1, keepdims=False)
        return beam_power(voltage, weight_block)

    return lax.map(one_channel, jnp.arange(turned.shape[2], dtype=jnp.int32))


def plain_on_device(voltages, weights):
    turned = lax.all_to_all(voltages, "gx", split_axis=3, concat_axis=1, tiled=True)
    partial_power_value = channel_powers(turned[0], weights)
    relaid = lax.all_to_all(partial_power_value, "gx", split_axis=2, concat_axis=0, tiled=True)
    return lax.psum_scatter(relaid, "ta", scatter_dimension=3, tiled=True)


def kernel(
    nx, ng, v_ref, w_hbm, turn_ref, mix_ref, gather_ref, out_ref,
    sbuf, vrecv, w_ref, pbuf, w_sem, vsend, vget, psend, pget,
):
    x = lax.axis_index("ta")
    g = lax.axis_index("gx")
    me = x * ng + g
    n = nx * ng
    rows = v_ref.shape[0] * v_ref.shape[1]
    chans = v_ref.shape[2] // ng
    half = v_ref.shape[3] // nx
    per = chans // CHUNKS
    group = ng // 2
    antennas2 = group * rows
    beams = w_ref.shape[3]

    w_copy = pltpu.make_async_copy(w_hbm, w_ref, w_sem)
    w_copy.start()

    barrier = pltpu.get_barrier_semaphore()

    def greet(i, _):
        d = lax.rem(me + i, n)
        pl.semaphore_signal(
            barrier, inc=1, device_id=(d // ng, lax.rem(d, ng)), device_id_type=MESH
        )
        return 0

    lax.fori_loop(1, n, greet, 0)

    def turn(b, _):
        start = pl.multiple_of(b * chans, chans)
        block = v_ref[:, :, pl.ds(start, chans), :].reshape(rows * chans, nx * half)
        turned = jnp.dot(turn_ref[...], block, preferred_element_type=jnp.float32)
        turned = turned.astype(jnp.bfloat16).reshape(CHUNKS, per, rows, nx * half)
        for k in range(nx):
            sbuf[:, k * ng + b] = turned[:, :, :, k * half : (k + 1) * half]
        return 0

    lax.fori_loop(0, ng, turn, 0)
    pl.semaphore_wait(barrier, n - 1)

    for k in range(CHUNKS):
        pltpu.make_async_copy(sbuf.at[k, me], vrecv.at[k, me], vget.at[k]).start()

        def send(i, _, k=k):
            d = lax.rem(me + i, n)
            pltpu.make_async_remote_copy(
                src_ref=sbuf.at[k, d],
                dst_ref=vrecv.at[k, me],
                send_sem=vsend.at[k],
                recv_sem=vget.at[k],
                device_id=(d // ng, lax.rem(d, ng)),
                device_id_type=MESH,
            ).start()
            return 0

        lax.fori_loop(1, n, send, 0)

    w_copy.wait()

    def chunk_step(k, _):
        pltpu.make_async_copy(vrecv.at[k], vrecv.at[k], vget.at[k]).wait()

        def channel(step, _):
            c = step // 2
            q = lax.rem(step, 2)
            col = k * per + c
            w = jnp.concatenate([w_ref[q, col, 0], w_ref[q, col, 1]], axis=1)
            power = None
            for h in range(nx):
                first = h * ng + q * group
                v = vrecv[k, pl.ds(first, group), c].reshape(antennas2, half)
                mixed = jnp.dot(mix_ref[...], v, preferred_element_type=jnp.float32)
                mixed = mixed.astype(jnp.bfloat16)
                re = jnp.dot(w, mixed[:antennas2], preferred_element_type=jnp.float32)
                im = jnp.dot(w, mixed[antennas2:], preferred_element_type=jnp.float32)
                part = re * re + im * im
                power = part if power is None else power + part
            own = beams // ng
            packs = own // 8
            power = power.reshape(ng, packs, 8, half)
            total = None
            for m in range(packs):
                p = power[:, m].reshape(ng * 8, half)
                high = p.astype(jnp.bfloat16)
                low = (p - high.astype(jnp.float32)).astype(jnp.bfloat16)
                t = jnp.dot(high, gather_ref[m], preferred_element_type=jnp.float32)
                t += jnp.dot(low, gather_ref[m], preferred_element_type=jnp.float32)
                total = t if total is None else total + t
            pbuf[k, :, q, c] = total.reshape(ng, 8, 128)
            return 0

        lax.fori_loop(0, 2 * per, channel, 0)

        pltpu.make_async_copy(pbuf.at[k, g], out_ref.at[g, k], pget).start()

        def send(i, _):
            d = lax.rem(g + i, ng)
            pltpu.make_async_remote_copy(
                src_ref=pbuf.at[k, d],
                dst_ref=out_ref.at[g, k],
                send_sem=psend,
                recv_sem=pget,
                device_id=(x, d),
                device_id_type=MESH,
            ).start()
            return 0

        lax.fori_loop(1, ng, send, 0)
        return 0

    lax.fori_loop(0, CHUNKS, chunk_step, 0)

    pltpu.make_async_copy(out_ref, out_ref, pget).wait()
    for k in range(CHUNKS):
        sent = sbuf.at[k, pl.ds(0, n - 1)]
        pltpu.make_async_copy(sent, sent, vsend.at[k]).wait()
    sent = pbuf.at[:, pl.ds(0, ng - 1)]
    pltpu.make_async_copy(sent, sent, psend).wait()


def spread_kernel(in_ref, out_ref):
    chunks, per = in_ref.shape[1], in_ref.shape[3]
    bins = out_ref.shape[3]
    for m in range(128 // bins):
        for k in range(chunks):
            for q in range(2):
                out_ref[k * per : (k + 1) * per, q, m * 8 : (m + 1) * 8, :] = in_ref[
                    0, k, q, :, :, m * bins : (m + 1) * bins
                ]


def on_device(nx, ng, voltages, weights):
    v = voltages[0]
    streams, parts, channels, samples = v.shape
    rows, chans, half = streams * parts, channels // ng, samples // nx
    per = chans // CHUNKS
    group = ng // 2
    antennas = group * streams
    beams = weights.shape[3]
    own = beams // ng
    packs = own // 8
    bins = half // 8

    i = jnp.arange(rows * chans)[:, None]
    j = jnp.arange(rows * chans)[None, :]
    turn = ((j % chans == i // rows) & (j // chans == i % rows)).astype(jnp.bfloat16)
    i = jnp.arange(4 * antennas)[:, None]
    j = jnp.arange(2 * antennas)[None, :]
    block = i // antennas
    wants = 2 * (i % antennas) + jnp.where((block == 0) | (block == 3), 0, 1)
    mix = jnp.where(j == wants, jnp.where(block == 1, -1.0, 1.0), 0.0).astype(jnp.bfloat16)
    m = jnp.arange(packs)[:, None, None]
    s = jnp.arange(half)[None, :, None]
    lane = jnp.arange(128)[None, None, :]
    gather = (lane == m * bins + s // 8).astype(jnp.bfloat16)

    vmem = pl.BlockSpec(memory_space=pltpu.VMEM)
    anywhere = pl.BlockSpec(memory_space=pl.ANY)
    packed = pl.pallas_call(
        functools.partial(kernel, nx, ng),
        out_shape=jax.ShapeDtypeStruct((ng, CHUNKS, 2, per, 8, 128), jnp.float32),
        in_specs=[vmem, anywhere, vmem, vmem, vmem],
        out_specs=anywhere,
        scratch_shapes=[
            pltpu.VMEM((CHUNKS, nx * ng, per, rows, half), jnp.bfloat16),
            pltpu.VMEM((CHUNKS, nx * ng, per, rows, half), jnp.bfloat16),
            pltpu.VMEM(weights.shape, jnp.bfloat16),
            pltpu.VMEM((CHUNKS, ng, 2, per, 8, 128), jnp.float32),
            pltpu.SemaphoreType.DMA,
            pltpu.SemaphoreType.DMA((CHUNKS,)),
            pltpu.SemaphoreType.DMA((CHUNKS,)),
            pltpu.SemaphoreType.DMA,
            pltpu.SemaphoreType.DMA,
        ],
        compiler_params=pltpu.CompilerParams(
            collective_id=0, has_side_effects=True, vmem_limit_bytes=56 * 1024 * 1024
        ),
    )(v, weights, turn, mix, gather)

    return pl.pallas_call(
        spread_kernel,
        grid=(ng,),
        out_shape=jax.ShapeDtypeStruct((channels, 2, own, bins), jnp.float32),
        in_specs=[pl.BlockSpec((1, CHUNKS, 2, per, 8, 128), lambda b: (b, 0, 0, 0, 0, 0))],
        out_specs=pl.BlockSpec((chans, 2, own, bins), lambda b: (b, 0, 0, 0)),
    )(packed)


def solution(mesh):
    nx, ng = mesh.shape["ta"], mesh.shape["gx"]

    def body(voltages, weights):
        _, streams, parts, channels, samples = voltages.shape
        rows, chans, half = streams * parts, channels // ng, samples // nx
        own = weights.shape[3] // ng
        fits = (
            nx == 2
            and rows % 16 == 0
            and chans % 16 == 0
            and half % 128 == 0
            and own % 8 == 0
            and (own // 8) * (half // 8) == 128
        )
        if fits:
            return on_device(nx, ng, voltages, weights)
        return plain_on_device(voltages, weights)

    in_specs = (P("ta", "gx", None, None, None), P(None, "gx", None, None, None))
    out_specs = P(None, None, "gx", "ta")
    return jax.shard_map(
        body, mesh=mesh, in_specs=in_specs, out_specs=out_specs, check_vma=False
    )
```

```python
import functools

import jax
import jax.numpy as jnp
import numpy as np
from jax import lax
from jax.experimental import pallas as pl
from jax.experimental.pallas import tpu as pltpu
from jax.sharding import PartitionSpec as P

BF16 = np.dtype(jnp.bfloat16)
MESH = pl.DeviceIdType.MESH
CHUNKS = 4


def beam_power(voltage, weight_block):
    antennas = weight_block.shape[3]
    beam_count = weight_block.shape[2]
    powers = []
    for side_index in range(2):
        real_w = weight_block[side_index, 0]
        imag_w = weight_block[side_index, 1]
        upper_rows = jnp.stack([real_w, -imag_w], axis=-1).reshape(beam_count, 2 * antennas)
        bottom_half_rows = jnp.stack([imag_w, real_w], axis=-1).reshape(beam_count, 2 * antennas)
        matrix = jnp.concatenate([upper_rows, bottom_half_rows], 0)
        signal = voltage[side_index * antennas : (side_index + 1) * antennas].reshape(
            2 * antennas, -1
        )
        beam_voltage_field = jnp.dot(matrix, signal, preferred_element_type=jnp.float32)
        power = (
            beam_voltage_field[:beam_count] * beam_voltage_field[:beam_count]
            + beam_voltage_field[beam_count:] * beam_voltage_field[beam_count:]
        )
        powers.append(power.reshape(beam_count, -1, 8).sum(-1))
    return jnp.stack(powers, 0)


def channel_powers(turned, weights):

    def one_channel(column):
        voltage = lax.dynamic_index_in_dim(turned, column, 2, keepdims=False)
        weight_block = lax.dynamic_index_in_dim(weights, column, 1, keepdims=False)
        return beam_power(voltage, weight_block)

    return lax.map(one_channel, jnp.arange(turned.shape[2], dtype=jnp.int32))


def plain_on_device(voltages, weights):
    turned = lax.all_to_all(voltages, "gx", split_axis=3, concat_axis=1, tiled=True)
    partial_power_value = channel_powers(turned[0], weights)
    relaid = lax.all_to_all(partial_power_value, "gx", split_axis=2, concat_axis=0, tiled=True)
    return lax.psum_scatter(relaid, "ta", scatter_dimension=3, tiled=True)


def kernel(
    nx, ng, v_ref, w_hbm, turn_ref, mix_ref, gather_ref, out_ref,
    sbuf, vrecv, w_ref, pbuf, w_sem, vsend, vget, psend, pget,
):
    x = lax.axis_index("ta")
    g = lax.axis_index("gx")
    me = x * ng + g
    n = nx * ng
    rows = v_ref.shape[0] * v_ref.shape[1]
    chans = v_ref.shape[2] // ng
    half = v_ref.shape[3] // nx
    per = chans // CHUNKS
    group = ng // 2
    antennas2 = group * rows
    beams = w_ref.shape[4]

    w_copy = pltpu.make_async_copy(w_hbm, w_ref, w_sem)
    w_copy.start()

    barrier = pltpu.get_barrier_semaphore()

    def greet(i, _):
        d = lax.rem(me + i, n)
        pl.semaphore_signal(
            barrier, inc=1, device_id=(d // ng, lax.rem(d, ng)), device_id_type=MESH
        )
        return 0

    lax.fori_loop(1, n, greet, 0)

    def turn(b, _):
        start = pl.multiple_of(b * chans, chans)
        block = v_ref[:, :, pl.ds(start, chans), :].reshape(rows * chans, nx * half)
        turned = jnp.dot(turn_ref[...], block, preferred_element_type=jnp.float32)
        turned = turned.astype(jnp.bfloat16).reshape(CHUNKS, per, rows, nx * half)
        for k in range(nx):
            sbuf[:, k * ng + b] = turned[:, :, :, k * half : (k + 1) * half]
        return 0

    lax.fori_loop(0, ng, turn, 0)
    pl.semaphore_wait(barrier, n - 1)

    for k in range(CHUNKS):
        pltpu.make_async_copy(sbuf.at[k, me], vrecv.at[k, me], vget.at[k]).start()

        def send(i, _, k=k):
            d = lax.rem(me + i, n)
            pltpu.make_async_remote_copy(
                src_ref=sbuf.at[k, d],
                dst_ref=vrecv.at[k, me],
                send_sem=vsend.at[k],
                recv_sem=vget.at[k],
                device_id=(d // ng, lax.rem(d, ng)),
                device_id_type=MESH,
            ).start()
            return 0

        lax.fori_loop(1, n, send, 0)

    w_copy.wait()

    def chunk_step(k, _):
        pltpu.make_async_copy(vrecv.at[k], vrecv.at[k], vget.at[k]).wait()

        def channel(step, _):
            c = step // 2
            q = lax.rem(step, 2)
            col = k * per + c
            w = w_ref[q, col].reshape(antennas2, beams).T
            power = None
            for h in range(nx):
                first = h * ng + q * group
                v = vrecv[k, pl.ds(first, group), c].reshape(antennas2, half)
                mixed = jnp.dot(mix_ref[...], v, preferred_element_type=jnp.float32)
                mixed = mixed.astype(jnp.bfloat16)
                re = jnp.dot(w, mixed[:antennas2], preferred_element_type=jnp.float32)
                im = jnp.dot(w, mixed[antennas2:], preferred_element_type=jnp.float32)
                part = re * re + im * im
                power = part if power is None else power + part
            own = beams // ng
            packs = own // 8
            power = power.reshape(ng, packs, 8, half)
            total = None
            for m in range(packs):
                p = power[:, m].reshape(ng * 8, half)
                high = p.astype(jnp.bfloat16)
                low = (p - high.astype(jnp.float32)).astype(jnp.bfloat16)
                t = jnp.dot(high, gather_ref[m], preferred_element_type=jnp.float32)
                t += jnp.dot(low, gather_ref[m], preferred_element_type=jnp.float32)
                total = t if total is None else total + t
            pbuf[k, :, q, c] = total.reshape(ng, 8, 128)
            return 0

        lax.fori_loop(0, 2 * per, channel, 0)

        pltpu.make_async_copy(pbuf.at[k, g], out_ref.at[:, g, k], pget).start()

        def send(i, _):
            d = lax.rem(g + i, ng)
            pltpu.make_async_remote_copy(
                src_ref=pbuf.at[k, d],
                dst_ref=out_ref.at[:, g, k],
                send_sem=psend,
                recv_sem=pget,
                device_id=(x, d),
                device_id_type=MESH,
            ).start()
            return 0

        lax.fori_loop(1, ng, send, 0)
        return 0

    lax.fori_loop(0, CHUNKS, chunk_step, 0)

    pltpu.make_async_copy(out_ref, out_ref, pget).wait()
    for k in range(CHUNKS):
        sent = sbuf.at[k, pl.ds(0, n - 1)]
        pltpu.make_async_copy(sent, sent, vsend.at[k]).wait()
    sent = pbuf.at[:, pl.ds(0, ng - 1)]
    pltpu.make_async_copy(sent, sent, psend).wait()


def spread_kernel(in_ref, out_ref):
    channels, bins = out_ref.shape[3], out_ref.shape[2]
    for r in range(8):
        lanes = in_ref[0, pl.ds(r, channels, stride=8), :].T
        for m in range(128 // bins):
            out_ref[0, m * 8 + r] = lanes[m * bins : (m + 1) * bins]


def on_device(nx, ng, voltages, weights):
    v = voltages[0]
    streams, parts, channels, samples = v.shape
    rows, chans, half = streams * parts, channels // ng, samples // nx
    per = chans // CHUNKS
    group = ng // 2
    antennas = group * streams
    beams = weights.shape[3]
    own = beams // ng
    packs = own // 8
    bins = half // 8

    i = np.arange(rows * chans)[:, None]
    j = np.arange(rows * chans)[None, :]
    turn = ((j % chans == i // rows) & (j // chans == i % rows)).astype(BF16)
    i = np.arange(4 * antennas)[:, None]
    j = np.arange(2 * antennas)[None, :]
    block = i // antennas
    wants = 2 * (i % antennas) + np.where((block == 0) | (block == 3), 0, 1)
    mix = np.where(j == wants, np.where(block == 1, -1.0, 1.0), 0.0).astype(BF16)
    m = np.arange(packs)[:, None, None]
    s = np.arange(half)[None, :, None]
    lane = np.arange(128)[None, None, :]
    gather = (lane == m * bins + s // 8).astype(BF16)

    turned_weights = jnp.swapaxes(weights, 3, 4)
    vmem = pl.BlockSpec(memory_space=pltpu.VMEM)
    anywhere = pl.BlockSpec(memory_space=pl.ANY)
    packed = pl.pallas_call(
        functools.partial(kernel, nx, ng),
        out_shape=jax.ShapeDtypeStruct((2, ng, CHUNKS, per, 8, 128), jnp.float32),
        in_specs=[vmem, anywhere, vmem, vmem, vmem],
        out_specs=anywhere,
        scratch_shapes=[
            pltpu.VMEM((CHUNKS, nx * ng, per, rows, half), jnp.bfloat16),
            pltpu.VMEM((CHUNKS, nx * ng, per, rows, half), jnp.bfloat16),
            pltpu.VMEM(turned_weights.shape, jnp.bfloat16),
            pltpu.VMEM((CHUNKS, ng, 2, per, 8, 128), jnp.float32),
            pltpu.SemaphoreType.DMA,
            pltpu.SemaphoreType.DMA((CHUNKS,)),
            pltpu.SemaphoreType.DMA((CHUNKS,)),
            pltpu.SemaphoreType.DMA,
            pltpu.SemaphoreType.DMA,
        ],
        compiler_params=pltpu.CompilerParams(
            collective_id=0, has_side_effects=True, vmem_limit_bytes=56 * 1024 * 1024
        ),
    )(v, turned_weights, turn, mix, gather)

    spread = pl.pallas_call(
        spread_kernel,
        grid=(2,),
        out_shape=jax.ShapeDtypeStruct((2, own, bins, channels), jnp.float32),
        in_specs=[pl.BlockSpec((1, channels * 8, 128), lambda q: (q, 0, 0))],
        out_specs=pl.BlockSpec((1, own, bins, channels), lambda q: (q, 0, 0, 0)),
    )(packed.reshape(2, channels * 8, 128))
    return spread.transpose(3, 0, 1, 2)


def solution(mesh):
    nx, ng = mesh.shape["ta"], mesh.shape["gx"]

    def body(voltages, weights):
        _, streams, parts, channels, samples = voltages.shape
        rows, chans, half = streams * parts, channels // ng, samples // nx
        own = weights.shape[3] // ng
        fits = (
            nx == 2
            and rows % 16 == 0
            and chans % 16 == 0
            and half % 128 == 0
            and own % 8 == 0
            and (own // 8) * (half // 8) == 128
        )
        if fits:
            return on_device(nx, ng, voltages, weights)
        return plain_on_device(voltages, weights)

    in_specs = (P("ta", "gx", None, None, None), P(None, "gx", None, None, None))
    out_specs = P(None, None, "gx", "ta")
    return jax.shard_map(
        body, mesh=mesh, in_specs=in_specs, out_specs=out_specs, check_vma=False
    )
```

```python
import functools

import jax
import jax.numpy as jnp
import numpy as np
from jax import lax
from jax.experimental import pallas as pl
from jax.experimental.pallas import tpu as pltpu
from jax.sharding import PartitionSpec as P

BF16 = np.dtype(jnp.bfloat16)
MESH = pl.DeviceIdType.MESH
CHUNKS = 4
PIECES = 4
LEAD = 2


def beam_power(voltage, weight_block):
    antennas = weight_block.shape[3]
    beam_count = weight_block.shape[2]
    powers = []
    for side_index in range(2):
        real_w = weight_block[side_index, 0]
        imag_w = weight_block[side_index, 1]
        upper_rows = jnp.stack([real_w, -imag_w], axis=-1).reshape(beam_count, 2 * antennas)
        bottom_half_rows = jnp.stack([imag_w, real_w], axis=-1).reshape(beam_count, 2 * antennas)
        matrix = jnp.concatenate([upper_rows, bottom_half_rows], 0)
        signal = voltage[side_index * antennas : (side_index + 1) * antennas].reshape(
            2 * antennas, -1
        )
        beam_voltage_field = jnp.dot(matrix, signal, preferred_element_type=jnp.float32)
        power = (
            beam_voltage_field[:beam_count] * beam_voltage_field[:beam_count]
            + beam_voltage_field[beam_count:] * beam_voltage_field[beam_count:]
        )
        powers.append(power.reshape(beam_count, -1, 8).sum(-1))
    return jnp.stack(powers, 0)


def channel_powers(turned, weights):

    def one_channel(column):
        voltage = lax.dynamic_index_in_dim(turned, column, 2, keepdims=False)
        weight_block = lax.dynamic_index_in_dim(weights, column, 1, keepdims=False)
        return beam_power(voltage, weight_block)

    return lax.map(one_channel, jnp.arange(turned.shape[2], dtype=jnp.int32))


def plain_on_device(voltages, weights):
    turned = lax.all_to_all(voltages, "gx", split_axis=3, concat_axis=1, tiled=True)
    partial_power_value = channel_powers(turned[0], weights)
    relaid = lax.all_to_all(partial_power_value, "gx", split_axis=2, concat_axis=0, tiled=True)
    return lax.psum_scatter(relaid, "ta", scatter_dimension=3, tiled=True)


def kernel(
    nx, ng, v_ref, w_hbm, turn_ref, mix_ref, gather_ref, out_ref,
    sbuf, vrecv, w_ref, pbuf,
    w_sem, wsend, wz, relay_sem, wx, vsend, vget, psend, pget,
):
    x = lax.axis_index("ta")
    g = lax.axis_index("gx")
    me = x * ng + g
    n = nx * ng
    rows = v_ref.shape[0] * v_ref.shape[1]
    chans = v_ref.shape[2] // ng
    half = v_ref.shape[3] // nx
    per = chans // CHUNKS
    group = ng // 2
    antennas2 = group * rows
    beams = w_ref.shape[4]
    side = g // group
    u = lax.rem(g, group)
    partner = lax.rem(g + group, ng)
    steps = 2 * CHUNKS
    dests = nx * group
    mine = x * group + u
    piece = chans // nx // PIECES

    w_copy = pltpu.make_async_copy(w_hbm.at[side], w_ref.at[0], w_sem)
    w_copy.start()

    barrier = pltpu.get_barrier_semaphore()

    def greet(i, _):
        d = lax.rem(me + i, n)
        pl.semaphore_signal(
            barrier, inc=1, device_id=(d // ng, lax.rem(d, ng)), device_id_type=MESH
        )
        return 0

    lax.fori_loop(1, n, greet, 0)

    def turn_side(which):
        base = lax.rem(which + side, 2) * CHUNKS

        def turn(i, _):
            start = pl.multiple_of((which * group + i) * chans, chans)
            block = v_ref[:, :, pl.ds(start, chans), :].reshape(rows * chans, nx * half)
            turned = jnp.dot(turn_ref[...], block, preferred_element_type=jnp.float32)
            turned = turned.astype(jnp.bfloat16).reshape(CHUNKS, per, rows, nx * half)
            for k in range(nx):
                sbuf[pl.ds(base, CHUNKS), k * group + i] = turned[
                    :, :, :, k * half : (k + 1) * half
                ]
            return 0

        lax.fori_loop(0, group, turn, 0)

    def send_voltages(k):
        pltpu.make_async_copy(sbuf.at[k, mine], vrecv.at[k, mine], vget.at[k]).start()

        def send(i, _):
            d = lax.rem(mine + i, dests)
            pltpu.make_async_remote_copy(
                src_ref=sbuf.at[k, d],
                dst_ref=vrecv.at[k, mine],
                send_sem=vsend.at[k],
                recv_sem=vget.at[k],
                device_id=(d // group, side * group + lax.rem(d, group)),
                device_id_type=MESH,
            ).start()
            return 0

        lax.fori_loop(1, dests, send, 0)

    def send_weights(i):
        span = pl.ds((x * PIECES + i) * piece, piece)
        pltpu.make_async_remote_copy(
            src_ref=w_hbm.at[1 - side, span],
            dst_ref=w_ref.at[1, span],
            send_sem=wsend,
            recv_sem=wz.at[i],
            device_id=(x, partner),
            device_id_type=MESH,
        ).start()

    def relay_weights(i):
        block = w_ref.at[1, pl.ds((x * PIECES + i) * piece, piece)]
        pltpu.make_async_copy(block, block, wz.at[i]).wait()
        pltpu.make_async_remote_copy(
            src_ref=block,
            dst_ref=block,
            send_sem=relay_sem,
            recv_sem=wx,
            device_id=(1 - x, g),
            device_id_type=MESH,
        ).start()

    turn_side(side)
    pl.semaphore_wait(barrier, n - 1)
    for k in range(LEAD):
        send_voltages(k)
        send_weights(k)
    turn_side(1 - side)
    w_copy.wait()

    def step(k, _):
        pltpu.make_async_copy(vrecv.at[k], vrecv.at[k], vget.at[k]).wait()

        @pl.when(k + LEAD < steps)
        def _():
            send_voltages(k + LEAD)

        @pl.when(k + LEAD < PIECES)
        def _():
            send_weights(k + LEAD)

        @pl.when((k >= 1) & (k <= PIECES))
        def _():
            relay_weights(k - 1)

        @pl.when(k == CHUNKS)
        def _():
            other = w_ref.at[1, pl.ds((1 - x) * PIECES * piece, PIECES * piece)]
            pltpu.make_async_copy(other, other, wx).wait()

        which = k // CHUNKS
        part_of = lax.rem(k, CHUNKS)

        def channel(c, _):
            w = w_ref[which, part_of * per + c].reshape(antennas2, beams).T
            power = None
            for h in range(nx):
                v = vrecv[k, h * group : (h + 1) * group, c].reshape(antennas2, half)
                mixed = jnp.dot(mix_ref[...], v, preferred_element_type=jnp.float32)
                mixed = mixed.astype(jnp.bfloat16)
                re = jnp.dot(w, mixed[:antennas2], preferred_element_type=jnp.float32)
                im = jnp.dot(w, mixed[antennas2:], preferred_element_type=jnp.float32)
                part = re * re + im * im
                power = part if power is None else power + part
            own = beams // ng
            packs = own // 8
            power = power.reshape(ng, packs, 8, half)
            total = None
            for m in range(packs):
                p = power[:, m].reshape(ng * 8, half)
                high = p.astype(jnp.bfloat16)
                low = (p - high.astype(jnp.float32)).astype(jnp.bfloat16)
                t = jnp.dot(high, gather_ref[m], preferred_element_type=jnp.float32)
                t += jnp.dot(low, gather_ref[m], preferred_element_type=jnp.float32)
                total = t if total is None else total + t
            pbuf[k, :, c] = total.reshape(ng, 8, 128)
            return 0

        lax.fori_loop(0, per, channel, 0)

        target = out_ref.at[side, lax.rem(g + which * group, ng), part_of]
        pltpu.make_async_copy(pbuf.at[k, g], target, pget).start()

        def send(i, _):
            d = lax.rem(g + i, ng)
            pltpu.make_async_remote_copy(
                src_ref=pbuf.at[k, d],
                dst_ref=target,
                send_sem=psend,
                recv_sem=pget,
                device_id=(x, d),
                device_id_type=MESH,
            ).start()
            return 0

        lax.fori_loop(1, ng, send, 0)
        return 0

    lax.fori_loop(0, steps, step, 0)

    pltpu.make_async_copy(out_ref, out_ref, pget).wait()
    for k in range(steps):
        sent = sbuf.at[k, pl.ds(0, dests - 1)]
        pltpu.make_async_copy(sent, sent, vsend.at[k]).wait()
    sent = pbuf.at[:, pl.ds(0, ng - 1)]
    pltpu.make_async_copy(sent, sent, psend).wait()
    sent = w_ref.at[1, pl.ds(0, PIECES * piece)]
    pltpu.make_async_copy(sent, sent, wsend).wait()
    pltpu.make_async_copy(sent, sent, relay_sem).wait()


def spread_kernel(in_ref, out_ref):
    channels, bins = out_ref.shape[3], out_ref.shape[2]
    for r in range(8):
        lanes = in_ref[0, pl.ds(r, channels, stride=8), :].T
        for m in range(128 // bins):
            out_ref[0, m * 8 + r] = lanes[m * bins : (m + 1) * bins]


def on_device(nx, ng, voltages, weights):
    v = voltages[0]
    streams, parts, channels, samples = v.shape
    rows, chans, half = streams * parts, channels // ng, samples // nx
    per = chans // CHUNKS
    group = ng // 2
    antennas = group * streams
    beams = weights.shape[3]
    own = beams // ng
    packs = own // 8
    bins = half // 8

    i = np.arange(rows * chans)[:, None]
    j = np.arange(rows * chans)[None, :]
    turn = ((j % chans == i // rows) & (j // chans == i % rows)).astype(BF16)
    i = np.arange(4 * antennas)[:, None]
    j = np.arange(2 * antennas)[None, :]
    block = i // antennas
    wants = 2 * (i % antennas) + np.where((block == 0) | (block == 3), 0, 1)
    mix = np.where(j == wants, np.where(block == 1, -1.0, 1.0), 0.0).astype(BF16)
    m = np.arange(packs)[:, None, None]
    s = np.arange(half)[None, :, None]
    lane = np.arange(128)[None, None, :]
    gather = (lane == m * bins + s // 8).astype(BF16)

    turned_weights = jnp.swapaxes(weights, 3, 4)
    vmem = pl.BlockSpec(memory_space=pltpu.VMEM)
    anywhere = pl.BlockSpec(memory_space=pl.ANY)
    packed = pl.pallas_call(
        functools.partial(kernel, nx, ng),
        out_shape=jax.ShapeDtypeStruct((2, ng, CHUNKS, per, 8, 128), jnp.float32),
        in_specs=[vmem, anywhere, vmem, vmem, vmem],
        out_specs=anywhere,
        scratch_shapes=[
            pltpu.VMEM((2 * CHUNKS, nx * group, per, rows, half), jnp.bfloat16),
            pltpu.VMEM((2 * CHUNKS, nx * group, per, rows, half), jnp.bfloat16),
            pltpu.VMEM(turned_weights.shape, jnp.bfloat16),
            pltpu.VMEM((2 * CHUNKS, ng, per, 8, 128), jnp.float32),
            pltpu.SemaphoreType.DMA,
            pltpu.SemaphoreType.DMA,
            pltpu.SemaphoreType.DMA((PIECES,)),
            pltpu.SemaphoreType.DMA,
            pltpu.SemaphoreType.DMA,
            pltpu.SemaphoreType.DMA((2 * CHUNKS,)),
            pltpu.SemaphoreType.DMA((2 * CHUNKS,)),
            pltpu.SemaphoreType.DMA,
            pltpu.SemaphoreType.DMA,
        ],
        compiler_params=pltpu.CompilerParams(
            collective_id=0, has_side_effects=True, vmem_limit_bytes=56 * 1024 * 1024
        ),
    )(v, turned_weights, turn, mix, gather)

    spread = pl.pallas_call(
        spread_kernel,
        grid=(2,),
        out_shape=jax.ShapeDtypeStruct((2, own, bins, channels), jnp.float32),
        in_specs=[pl.BlockSpec((1, channels * 8, 128), lambda q: (q, 0, 0))],
        out_specs=pl.BlockSpec((1, own, bins, channels), lambda q: (q, 0, 0, 0)),
    )(packed.reshape(2, channels * 8, 128))
    return spread.transpose(3, 0, 1, 2)


def solution(mesh):
    nx, ng = mesh.shape["ta"], mesh.shape["gx"]

    def body(voltages, weights):
        _, streams, parts, channels, samples = voltages.shape
        rows, chans, half = streams * parts, channels // ng, samples // nx
        own = weights.shape[3] // ng
        fits = (
            nx == 2
            and rows % 16 == 0
            and chans % 16 == 0
            and half % 128 == 0
            and own % 8 == 0
            and (own // 8) * (half // 8) == 128
        )
        if fits:
            return on_device(nx, ng, voltages, weights)
        return plain_on_device(voltages, weights)

    in_specs = (P("ta", "gx", None, None, None), P(None, "gx", None, None, None))
    out_specs = P(None, None, "gx", "ta")
    return jax.shard_map(
        body, mesh=mesh, in_specs=in_specs, out_specs=out_specs, check_vma=False
    )
```
